32 devices in a mesh: section: 8 (over z, x), tensor: 2 (over core), dp: 2 (over y).
Axes of the slice: x: 2, y: 2, z: 4, core: 2. Of those that a mesh axis runs over, the one named last changes fastest.
Arguments:
- forward_input: bfloat16 [8, 256, 4096], P('section', 'dp', 'tensor'), may hold values from -6 to 6
- entering_input: bfloat16 [256, 4096], P('dp', 'tensor'), may hold values from -6 to 6
- stored_input: bfloat16 [2, 8, 256, 4096], P(None, 'section', 'dp', 'tensor'), may hold values from -6 to 6
- output_gradient: bfloat16 [8, 256, 4096], P('section', 'dp', 'tensor'), may hold values from -6 to 6
- last_gradient: bfloat16 [256, 4096], P('dp', 'tensor'), may hold values from -6 to 6
- norm_weight: bfloat16 [8, 4096], P('section', 'tensor'), may hold values from 0.25 to 1.75
- frozen_weight: bfloat16 [8, 4096, 4096], P('section', 'dp', 'tensor'), may hold values from -1 to 2
- adapter_down: bfloat16 [8, 4096, 128], P('section', 'tensor'), may hold values from -0.09375 to 0.09375
- adapter_up: bfloat16 [8, 128, 4096], P('section', None, 'tensor'), may hold values from -0.5 to 0.5
- project: bfloat16 [8, 4096, 32], P('section', 'tensor'), may hold values from -0.013671875 to 0.013671875
- example_token_counts: int32 [2, 9, 3], P('dp'), may hold values from 1 to 64, 128 in all within a row
- sketch_owner_rows: int32 [2, 27], P('dp'), may hold values from 0 to 26, each once within a row
Outputs:
- fwd_out: bfloat16 [8, 256, 4096], P('section', 'dp', 'tensor')
- grad_out: bfloat16 [8, 256, 4096], P('section', 'dp', 'tensor')
- sketches: float32 [54, 4096], P('dp', 'section')
The draws below stay inside these ranges and needn't reach their ends.
Inputs may be any that keep to these rules, and one draw needn't show every extreme that they name: `example_token_counts`: each micro-batch of each replica holds 3 examples whose lengths sum to 128, the longest exactly 64. `sketch_owner_rows`: within each replica every owner row appears exactly once.
All inputs are finite; a program needn't handle non-finite values.
Results may differ from the reference program's by a relative error of at most 0.025.
Values may be sent and summed in bfloat16 or wider, within the bound.
A program may use at most 64 MiB of HBM per device.

```python
import math
import jax
import jax.numpy as jnp
import numpy as np
from jax import lax

MODEL_WIDTH = 4096
ADAPTER_RANK = 128
SKETCH_COLUMNS = 32
PACKED_EXAMPLES = 3
TOK = 128
TOK_ALL = 256
BATCHES = 9
N_SECTION = 8
N_TENSOR = 2
N_DP = 2


def unit_draw(key, shape):
    return jax.random.normal(key, shape, jnp.float32)


def shared_batches(key):
    return unit_draw(jax.random.fold_in(key, 4111), (N_SECTION + 1, TOK_ALL, MODEL_WIDTH))


def draw_stored_input(key, part):
    common = shared_batches(key)
    first = 0.8 * common[:N_SECTION] + 0.6 * unit_draw(jax.random.fold_in(key, 4201), (N_SECTION, TOK_ALL, MODEL_WIDTH))
    second = 0.8 * common[1:] + 0.6 * unit_draw(jax.random.fold_in(key, 4202), (N_SECTION, TOK_ALL, MODEL_WIDTH))
    stacked = jnp.stack([first, second])
    return jnp.clip(stacked, -6.0, 6.0).astype(jnp.bfloat16)


def draw_output_gradient(key, part):
    common = shared_batches(key)
    values = 0.9 * common[:N_SECTION] + 0.44 * unit_draw(jax.random.fold_in(key, 4211), (N_SECTION, TOK_ALL, MODEL_WIDTH))
    return jnp.clip(values, -6.0, 6.0).astype(jnp.bfloat16)


def draw_last_gradient(key, part):
    common = shared_batches(key)
    values = 0.9 * common[N_SECTION] + 0.44 * unit_draw(jax.random.fold_in(key, 4221), (TOK_ALL, MODEL_WIDTH))
    return jnp.clip(values, -6.0, 6.0).astype(jnp.bfloat16)


def draw_frozen_weight(key, part):
    random_part = jnp.clip(unit_draw(jax.random.fold_in(key, 4301), (N_SECTION, MODEL_WIDTH, MODEL_WIDTH)), -4.0, 4.0)
    identity = jnp.eye(MODEL_WIDTH, dtype=jnp.float32)[None]
    values = identity + 0.8 * MODEL_WIDTH ** (-0.5) * random_part
    return values.astype(jnp.bfloat16)


def block_scale(own_key, shape, pieces, least, top_value):
    factor_of, own = 1.0, jax.random.fold_in(own_key, 6)
    for position, blocks in pieces:
        heights = jnp.exp(jax.random.uniform(jax.random.fold_in(own, position), (blocks,), jnp.float32, least / len(pieces), top_value / len(pieces)))
        factor_of = factor_of * jnp.repeat(heights, shape[position] // blocks).reshape([-1 if axis == position else 1 for axis in range(len(shape))])
    return factor_of


def length_profile(amount, total, bound, skew):
    weights = [(1 << 20) // math.isqrt(standing ** skew) + 1 for standing in range(2, amount + 1)]
    spare, given = total - bound - (amount - 1), [1] * (amount - 1)
    while spare > 0:
        candidates = [i for i in range(amount - 1) if given[i] < bound]
        pool, remaining = sum([weights[i] for i in candidates]), spare
        for i in candidates:
            extra = min(bound - given[i], max(1, remaining * weights[i] // pool), spare)
            given[i] = given[i] + extra
            spare = spare - extra
    return np.array([bound] + given)


def ragged(own_key, number_of, total, most, slope):
    if number_of == 2:
        one = jax.random.randint(own_key, (), max(1, total - most), min(most, total - 1) + 1)
        return jnp.stack([one, total - one])
    sizes = jnp.asarray(length_profile(number_of, total, most, slope), jnp.int32)
    twos = (number_of - 1) // 2
    giver, sink = sizes[1:1 + 2 * twos:2], sizes[2:2 + 2 * twos:2]
    margin = jnp.minimum(giver - 1, most - sink)
    moved = jax.random.randint(jax.random.fold_in(own_key, 1), (twos,), 0, 1 << 20) % (margin + 1)
    sizes = sizes.at[1:1 + 2 * twos:2].set(giver - moved).at[2:2 + 2 * twos:2].set(sink + moved)
    return sizes[jax.random.permutation(jax.random.fold_in(own_key, 2), number_of)]


def scatter_about(rng, extent, deviation, bound, cuts=(), kind=jnp.bfloat16):
    factor_of = block_scale(rng, extent, cuts, -0.22, 0.18) if cuts else 1.0
    drawn = jax.random.normal(rng, extent, jnp.float32) * deviation * factor_of
    return jnp.minimum(jnp.maximum(drawn, -bound), bound).astype(kind)


def setup_inputs(seed: int = 0) -> dict:
    key_list = jax.random.split(jax.random.key(seed), 13)
    forward_input = scatter_about(key_list[0], (N_SECTION, TOK_ALL, MODEL_WIDTH), 1.0, 6.0, ((0, 8), (1, 2), (2, 2)))
    entering_input = scatter_about(key_list[1], (TOK_ALL, MODEL_WIDTH), 1.0, 6.0, ((0, 2), (1, 2)))
    stored_input = draw_stored_input(jax.random.fold_in(key_list[12], 71), 0)
    output_gradient = draw_output_gradient(jax.random.fold_in(key_list[12], 71), 0)
    last_gradient = draw_last_gradient(jax.random.fold_in(key_list[12], 71), 0)
    norm_weight = jnp.clip(1.0 + 0.15 * jax.random.normal(key_list[5], (N_SECTION, MODEL_WIDTH), jnp.float32), 0.25, 1.75).astype(jnp.bfloat16)
    frozen_weight = draw_frozen_weight(jax.random.fold_in(key_list[12], 71), 0)
    adapter_down = scatter_about(key_list[7], (N_SECTION, MODEL_WIDTH, ADAPTER_RANK), MODEL_WIDTH ** -0.5, 0.09375, ((0, 8), (1, 2)))
    adapter_up = scatter_about(key_list[8], (N_SECTION, ADAPTER_RANK, MODEL_WIDTH), ADAPTER_RANK ** -0.5, 0.5, ((0, 8), (2, 2)))
    project = scatter_about(key_list[9], (N_SECTION, MODEL_WIDTH, SKETCH_COLUMNS), (MODEL_WIDTH * TOK // PACKED_EXAMPLES) ** -0.5, 0.013671875, ((0, 8), (1, 2)))
    example_token_counts = jax.vmap(lambda own: ragged(own, PACKED_EXAMPLES, TOK, TOK // 2, 0))(jax.random.split(key_list[10], N_DP * BATCHES)).reshape((N_DP, BATCHES, PACKED_EXAMPLES)).astype(jnp.int32)
    sketch_owner_rows = jax.vmap(lambda own: jax.random.permutation(own, BATCHES * PACKED_EXAMPLES))(jax.random.split(key_list[11], N_DP)).reshape((N_DP, BATCHES * PACKED_EXAMPLES)).astype(jnp.int32)
    return dict(forward_input=forward_input, entering_input=entering_input, stored_input=stored_input, output_gradient=output_gradient, last_gradient=last_gradient, norm_weight=norm_weight, frozen_weight=frozen_weight, adapter_down=adapter_down, adapter_up=adapter_up, project=project, example_token_counts=example_token_counts, sketch_owner_rows=sketch_owner_rows)


ADAPTER_SCALE = 2.0
NORM_EPS = 1e-05

def normalize(hidden, norm_scale):
    wide = hidden.astype(jnp.float32)
    inv_rms = lax.rsqrt(lax.optimization_barrier(jnp.mean(wide * wide, axis=1, keepdims=True)) + NORM_EPS)
    normed = (wide * inv_rms * norm_scale.astype(jnp.float32)[None, :]).astype(jnp.bfloat16)
    return (wide, inv_rms, normed)

def forward_layer(hidden, norm_scale, weight, down_factor, up_factor):
    wide, inv_rms, normed = normalize(hidden, norm_scale)
    adapter_input = jnp.dot(normed, down_factor, preferred_element_type=jnp.float32).astype(jnp.bfloat16)
    combined_output = jnp.dot(normed, weight, preferred_element_type=jnp.float32)
    combined_output = combined_output + ADAPTER_SCALE * jnp.dot(adapter_input, up_factor, preferred_element_type=jnp.float32)
    return (wide + combined_output).astype(jnp.bfloat16)

def backward_layer(hidden, cotangent, norm_scale, weight, down_factor, up_factor, proj):
    wide, inv_rms, normed = normalize(hidden, norm_scale)
    adapter_input = jnp.dot(normed, down_factor, preferred_element_type=jnp.float32).astype(jnp.bfloat16)
    adapter_gradient = jnp.dot(cotangent, up_factor.T, preferred_element_type=jnp.float32).astype(jnp.bfloat16)
    sketch_cols = jnp.dot(cotangent, proj, preferred_element_type=jnp.float32)
    token_rows = cotangent.shape[0]
    grouped = cotangent.astype(jnp.float32).reshape(token_rows, N_TENSOR, -1)
    weight_groups = weight.astype(jnp.float32).reshape(MODEL_WIDTH, N_TENSOR, -1)
    partials = jnp.einsum('tnc,dnc->ntd', grouped, weight_groups, precision=lax.Precision.HIGHEST)
    rounded = lax.optimization_barrier(partials.astype(jnp.bfloat16))
    reduced_sum = lax.optimization_barrier(jnp.sum(rounded.astype(jnp.float32), axis=0))
    normed_gradient = reduced_sum + ADAPTER_SCALE * jnp.dot(adapter_gradient, down_factor.T, preferred_element_type=jnp.float32)
    scaled = norm_scale.astype(jnp.float32)[None, :] * normed_gradient
    inner_sum = lax.optimization_barrier(jnp.mean(wide * scaled, axis=1, keepdims=True))
    back = cotangent.astype(jnp.float32) + inv_rms * (scaled - wide * inv_rms * inv_rms * inner_sum)
    return (back.astype(jnp.bfloat16), adapter_input, sketch_cols)

def example_sketch(adapter_input, sketch_cols, example_lengths):
    seg_ends = jnp.cumsum(example_lengths)
    seg_starts = seg_ends - example_lengths
    positions = lax.broadcasted_iota(jnp.int32, (adapter_input.shape[0], example_lengths.shape[0]), 0).astype(example_lengths.dtype)
    member = ((positions >= seg_starts[None, :]) & (positions < seg_ends[None, :])).astype(jnp.float32)
    part = jnp.einsum('tj,tr,tk->jrk', member, adapter_input.astype(jnp.float32), sketch_cols, precision=lax.Precision.HIGHEST)
    return ADAPTER_SCALE * part.reshape(example_lengths.shape[0], -1)

def reference(forward_input, entering_input, stored_input, output_gradient, last_gradient, norm_weight, frozen_weight, adapter_down, adapter_up, project, example_token_counts, sketch_owner_rows):
    layer_weights = (norm_weight, frozen_weight, adapter_down, adapter_up)

    def run_forward(packed):
        hidden, norm_scale, weight, down_factor, up_factor = packed
        return forward_layer(hidden, norm_scale, weight, down_factor, up_factor)

    def run_backward(packed):
        hidden, cotangent, norm_scale, weight, down_factor, up_factor, proj, example_lengths = packed
        back, adapter_input, sketch_cols = backward_layer(hidden, cotangent, norm_scale, weight, down_factor, up_factor, proj)
        parts = []
        for replica in range(N_DP):
            lower = replica * TOK
            parts.append(example_sketch(adapter_input[lower:lower + TOK], sketch_cols[lower:lower + TOK], example_lengths[replica]))
        return (back, jnp.stack(parts))
    lengths_first = jnp.swapaxes(example_token_counts[:, :N_SECTION], 0, 1)
    lengths_second = jnp.swapaxes(example_token_counts[:, 1:], 0, 1)
    first_out = lax.map(run_forward, (forward_input,) + layer_weights)
    back_first, sketch_first = lax.map(run_backward, (stored_input[0], output_gradient) + layer_weights + (project, lengths_first))
    entering = jnp.concatenate([entering_input[None], first_out[:-1]], 0)
    upstream = jnp.concatenate([back_first[1:], last_gradient[None]], 0)
    later_output = lax.map(run_forward, (entering,) + layer_weights)
    second_backward, sketch_second = lax.map(run_backward, (stored_input[1], upstream) + layer_weights + (project, lengths_second))
    batch_lengths = jnp.zeros((N_SECTION + 1, N_DP, PACKED_EXAMPLES, ADAPTER_RANK * SKETCH_COLUMNS), jnp.float32)
    batch_lengths = batch_lengths.at[:N_SECTION].add(sketch_first)
    batch_lengths = batch_lengths.at[1:].add(sketch_second)
    batch_lengths = jnp.swapaxes(batch_lengths, 0, 1).reshape(N_DP, (N_SECTION + 1) * PACKED_EXAMPLES, ADAPTER_RANK * SKETCH_COLUMNS)
    replica_ids = jnp.arange(N_DP).astype(jnp.int32)[:, None]
    located_rows = jnp.zeros_like(batch_lengths).at[replica_ids, sketch_owner_rows.astype(jnp.int32)].set(batch_lengths)
    return (later_output, second_backward, located_rows.reshape(-1, ADAPTER_RANK * SKETCH_COLUMNS))
```

```python
import functools

import jax
import jax.numpy as jnp
from jax import lax
from jax.experimental import pallas as pl
from jax.experimental.pallas import tpu as pltpu
from jax.sharding import PartitionSpec as P

MODEL_WIDTH = 4096


ADAPTER_SCALE = 2.0
NORM_EPS = 1e-05


def shifted(value, axis, steps):
    count = lax.axis_size(axis)
    initial, last = (max(0, -steps), min(count, count - steps))
    return lax.ppermute(value, axis, [(source, source + steps) for source in range(initial, last)])


def normalize(hidden, norm_scale):
    wide = hidden.astype(jnp.float32)
    squares = lax.psum(jnp.sum(wide * wide, axis=1), "tensor")
    inv_rms = lax.rsqrt(squares / MODEL_WIDTH + NORM_EPS)[:, None]
    normed = (wide * inv_rms * norm_scale.astype(jnp.float32)[None, :]).astype(jnp.bfloat16)
    return (wide, inv_rms, normed)


def forward_layer(hidden, norm_scale, full_weight, down_factor, up_factor):
    wide, inv_rms, normed = normalize(hidden, norm_scale)
    full_normed = lax.all_gather(normed, "tensor", axis=1, tiled=True)
    adapter_input = lax.psum(
        jnp.dot(normed, down_factor, preferred_element_type=jnp.float32).astype(jnp.bfloat16),
        "tensor",
    )
    frozen_output = jnp.dot(full_normed, full_weight, preferred_element_type=jnp.float32)
    combined_output = frozen_output + ADAPTER_SCALE * jnp.dot(
        adapter_input, up_factor, preferred_element_type=jnp.float32
    )
    return (wide + combined_output).astype(jnp.bfloat16)


def backward_layer(hidden, cotangent, norm_scale, full_weight, down_factor, up_factor, proj):
    wide, inv_rms, normed = normalize(hidden, norm_scale)
    contract_last = (((1,), (1,)), ((), ()))
    adapter_input, adapter_gradient, sketch_cols = (
        lax.psum(
            jnp.dot(normed, down_factor, preferred_element_type=jnp.float32).astype(jnp.bfloat16),
            "tensor",
        ).astype(jnp.float32),
        lax.psum(
            lax.dot_general(
                cotangent, up_factor, contract_last, preferred_element_type=jnp.float32
            ).astype(jnp.bfloat16),
            "tensor",
        ).astype(jnp.float32),
        lax.psum(
            jnp.dot(cotangent, proj, preferred_element_type=jnp.float32).astype(jnp.bfloat16),
            "tensor",
        ).astype(jnp.float32),
    )
    adapter_input = adapter_input.astype(jnp.bfloat16)
    adapter_gradient = adapter_gradient.astype(jnp.bfloat16)
    partials = lax.dot_general(
        cotangent, full_weight, contract_last, preferred_element_type=jnp.float32
    )
    reduced_sum = lax.psum_scatter(
        partials.astype(jnp.bfloat16), "tensor", scatter_dimension=1, tiled=True
    ).astype(jnp.float32)
    normed_gradient = reduced_sum + ADAPTER_SCALE * lax.dot_general(
        adapter_gradient, down_factor, contract_last, preferred_element_type=jnp.float32
    )
    scaled = norm_scale.astype(jnp.float32)[None, :] * normed_gradient
    inner_sum = lax.psum(jnp.sum(wide * scaled, axis=1), "tensor")[:, None] / MODEL_WIDTH
    back = cotangent.astype(jnp.float32) + inv_rms * (scaled - wide * inv_rms * inv_rms * inner_sum)
    return (back.astype(jnp.bfloat16), adapter_input, sketch_cols)


def example_sketch(adapter_input, sketch_cols, example_lengths):
    seg_ends = jnp.cumsum(example_lengths)
    seg_starts = seg_ends - example_lengths
    positions = lax.broadcasted_iota(
        jnp.int32, (adapter_input.shape[0], example_lengths.shape[0]), 0
    )
    member = ((positions >= seg_starts[None, :]) & (positions < seg_ends[None, :])).astype(
        jnp.float32
    )
    masked = (adapter_input.astype(jnp.float32)[:, None, :] * member[:, :, None]).reshape(
        adapter_input.shape[0], -1
    )
    part = lax.dot_general(
        masked,
        sketch_cols,
        (((0,), (0,)), ((), ())),
        precision=lax.Precision.HIGHEST,
        preferred_element_type=jnp.float32,
    )
    return ADAPTER_SCALE * part.reshape(example_lengths.shape[0], -1)


def per_device(
    forward_input,
    entering_input,
    stored_input,
    output_gradient,
    last_gradient,
    norm_weight,
    frozen_weight,
    adapter_down,
    adapter_up,
    project,
    example_token_counts,
    sketch_owner_rows,
):
    sections = lax.axis_size("section")
    section_index = lax.axis_index("section")
    norm_scale = norm_weight[0]
    weight_rows = frozen_weight[0]
    down_factor = adapter_down[0]
    up_factor = adapter_up[0]
    proj = project[0]
    full_weight = lax.all_gather(weight_rows, "dp", axis=0, tiled=True)
    first_out = forward_layer(forward_input[0], norm_scale, full_weight, down_factor, up_factor)
    back_first, adapter_first, cols_first = backward_layer(
        stored_input[0, 0],
        output_gradient[0],
        norm_scale,
        full_weight,
        down_factor,
        up_factor,
        proj,
    )
    arrived = shifted(first_out, "section", 1)
    returned = shifted(back_first, "section", -1)
    entering = jnp.where(section_index == 0, entering_input, arrived)
    upstream = jnp.where(section_index == sections - 1, last_gradient, returned)
    later_output = forward_layer(entering, norm_scale, full_weight, down_factor, up_factor)
    second_backward, adapter_second, cols_second = backward_layer(
        stored_input[1, 0], upstream, norm_scale, full_weight, down_factor, up_factor, proj
    )
    lengths_all = example_token_counts[0]
    batch_count = lengths_all.shape[0]
    seg_count = lengths_all.shape[1]
    lengths_first = lax.dynamic_index_in_dim(lengths_all, section_index, 0, keepdims=False)
    lengths_second = lax.dynamic_index_in_dim(lengths_all, section_index + 1, 0, keepdims=False)
    sketch_first = example_sketch(adapter_first, cols_first, lengths_first)
    sketch_second = example_sketch(adapter_second, cols_second, lengths_second)
    stacked = jnp.concatenate([sketch_first, sketch_second], 0)[None]
    pieces = lax.all_to_all(
        stacked.astype(jnp.bfloat16), "section", split_axis=2, concat_axis=0, tiled=True
    ).astype(stacked.dtype)
    early_part = jnp.pad(pieces[:, :seg_count], ((0, 1), (0, 0), (0, 0)))
    late_part = jnp.pad(pieces[:, seg_count:], ((1, 0), (0, 0), (0, 0)))
    gathered = (early_part + late_part).reshape(batch_count * seg_count, -1)
    row_ids = sketch_owner_rows[0]
    targets = lax.broadcasted_iota(jnp.int32, (row_ids.shape[0], row_ids.shape[0]), 1)
    placement_table = (row_ids[:, None] == targets).astype(jnp.float32)
    sketches = lax.dot_general(
        placement_table,
        gathered,
        (((0,), (0,)), ((), ())),
        precision=lax.Precision.HIGHEST,
        preferred_element_type=jnp.float32,
    )
    return (later_output[None], second_backward[None], sketches)


MESH = pl.DeviceIdType.MESH
CONTRACT_LAST = (((1,), (1,)), ((), ()))
ROWS = 16
TILE = 256

COPIES = (
    "norm",
    "down",
    "up",
    "proj",
    "h1",
    "g1",
    "s1",
    "s2",
    "last",
    "g1y",
    "shift_f",
    "shift_b0",
    "shift_b1",
    "h2",
    "g20",
    "g21",
    "g2y0",
    "g2y1",
    "nin1",
    "nfw1",
    "nin2",
    "nfw2",
    "fa1",
    "fb1",
    "fa2",
    "fb2",
    "pb1",
    "pb2",
    "po1",
    "po2",
    "dn1",
    "dn2",
    "back",
)


def window_kernel(
    sections,
    h_in,
    enter_in,
    stored_in,
    g_in,
    last_in,
    norm_in,
    w_in,
    down_in,
    up_in,
    proj_in,
    counts,
    owners,
    out_f,
    out_b,
    out_s,
    w,
    nwf,
    downf,
    upf,
    projf,
    h1f,
    h2f,
    s1f,
    s2f,
    g1f,
    g2f,
    g1o,
    g2o,
    normed,
    scratch_n,
    other_in,
    f_send,
    f_recv,
    f_own,
    o1,
    pb,
    pbr,
    po,
    por,
    sb,
    dn,
    lora,
    bk,
    bkr,
    inv_f,
    inv_1,
    inv_2,
    sk,
    skr,
    send_sem,
    recv_sem,
    sk_send,
    sk_recv,
    local_sem,
):
    s, t, d = lax.axis_index("section"), lax.axis_index("tensor"), lax.axis_index("dp")
    tokens, width = h_in.shape
    half = tokens // 2
    features = 2 * width
    segs = counts.shape[1]
    final = sections - 1
    other_t, other_d = 1 - t, 1 - d
    partner = {"tensor": other_t}
    peer = {"dp": other_d}
    cross = {"tensor": other_t, "dp": other_d}
    mine = pl.ds(pl.multiple_of(t * half, half), half)
    theirs = pl.ds(pl.multiple_of(other_t * half, half), half)

    def remote(name, src, dst, device, tick=None):
        index = COPIES.index(name if tick is None else name + str(tick))
        return pltpu.make_async_remote_copy(
            src_ref=src,
            dst_ref=dst,
            send_sem=send_sem.at[index],
            recv_sem=recv_sem.at[index],
            device_id=device,
            device_id_type=MESH,
        )

    def f32(value):
        return value.astype(jnp.float32)

    local = [
        pltpu.make_async_copy(src, dst, local_sem.at[i])
        for i, (src, dst) in enumerate(
            [
                (h_in, h1f.at[t]),
                (norm_in, nwf.at[t]),
                (stored_in.at[0], s1f.at[t]),
                (g_in, g1f.at[t]),
                (down_in, downf.at[t]),
                (up_in, upf.at[t]),
                (proj_in, projf.at[t]),
                (stored_in.at[1], s2f.at[t]),
                (w_in, w),
            ]
        )
    ]
    for copy in local:
        copy.start()
    enter_copy = pltpu.make_async_copy(enter_in, h2f.at[t], local_sem.at[9])
    last_copy = pltpu.make_async_copy(last_in, g2f.at[t], local_sem.at[10])

    @pl.when(s == 0)
    def _():
        enter_copy.start()

    @pl.when(s == final)
    def _():
        last_copy.start()

    barrier = pltpu.get_barrier_semaphore()
    for device in (partner, peer, cross):
        pl.semaphore_signal(barrier, inc=1, device_id=device, device_id_type=MESH)
    for step in range(1, sections):
        pl.semaphore_signal(
            barrier,
            inc=1,
            device_id={"section": lax.rem(s + step, sections)},
            device_id_type=MESH,
        )
    pl.semaphore_wait(barrier, 3 + sections - 1)

    g1y = remote("g1y", g_in, g1o, peer)
    h1c = remote("h1", h_in, h1f.at[t], partner)
    normc = remote("norm", norm_in, nwf.at[t], partner)
    s1c = remote("s1", stored_in.at[0], s1f.at[t], partner)
    downc = remote("down", down_in, downf.at[t], partner)
    g1c = remote("g1", g_in, g1f.at[t], partner)
    upc = remote("up", up_in, upf.at[t], partner)
    projc = remote("proj", proj_in, projf.at[t], partner)
    s2c = remote("s2", stored_in.at[1], s2f.at[t], partner)
    early = [h1c, normc, g1y, s1c, downc, g1c, upc, projc, s2c]
    for copy in early:
        copy.start()
    lastc = remote("last", last_in, g2f.at[t], partner)

    @pl.when(s == final)
    def _():
        lastc.start()

    def normalize_into(hidden, inv, dst):
        def body(i, carry):
            rows = pl.ds(pl.multiple_of(i * ROWS, ROWS), ROWS)
            total = jnp.zeros((ROWS, 1), jnp.float32)
            for b in range(2):
                wide = f32(hidden[b, rows, :])
                total = total + jnp.sum(wide * wide, axis=1, keepdims=True)
            scale = lax.rsqrt(total / features + NORM_EPS)
            inv[rows, :] = jnp.broadcast_to(scale, (ROWS, inv.shape[1]))
            for b in range(2):
                dst[b, rows, :] = (f32(hidden[b, rows, :]) * scale * f32(nwf[b])).astype(
                    jnp.bfloat16
                )
            return carry

        lax.fori_loop(0, tokens // ROWS, body, 0)

    def both(lhs, rhs):
        return (
            jnp.dot(lhs[0], rhs[0], preferred_element_type=jnp.float32)
            + jnp.dot(lhs[1], rhs[1], preferred_element_type=jnp.float32)
        )

    def forward_send(hidden, inv, tick):
        normalize_into(hidden, inv, normed)
        copy = remote("nin", normed.at[other_d, mine], other_in.at[tick - 1, mine], peer, tick)
        copy.start()
        return copy

    def forward_relay(copy, tick):
        copy.wait_recv()
        part = other_in.at[tick - 1, mine]
        relay = remote("nfw", part, part, partner, tick)
        relay.start()
        return relay

    def forward_other(relay, tick):
        relay.wait_recv()
        copies = []
        for name, first in (("fa", 0), ("fb", width // 2)):

            def body(n, carry, first=first):
                cols = pl.ds(pl.multiple_of(first + n * TILE, TILE), TILE)
                f_send[tick - 1, :, cols] = jnp.dot(
                    other_in[tick - 1], w[:, cols], preferred_element_type=jnp.float32
                ).astype(jnp.bfloat16)
                return carry

            lax.fori_loop(0, width // 2 // TILE, body, 0)
            cols = pl.ds(first, width // 2)
            copy = remote(
                name, f_send.at[tick - 1, :, cols], f_recv.at[tick - 1, :, cols], peer, tick
            )
            copy.start()
            copies.append(copy)
        return copies

    def forward_own(hidden, adapter):
        def body(n, carry):
            cols = pl.ds(pl.multiple_of(n * TILE, TILE), TILE)
            f_own[:, cols] = (
                f32(hidden[t, :, cols])
                + jnp.dot(normed[d], w[:, cols], preferred_element_type=jnp.float32)
                + ADAPTER_SCALE
                * jnp.dot(adapter, upf[t, :, cols], preferred_element_type=jnp.float32)
            )
            return carry

        lax.fori_loop(0, width // TILE, body, 0)

    def forward_finish(copies, dst, tick):
        for part, copy in enumerate(copies):
            copy.wait_recv()
            cols = pl.ds(part * (width // 2), width // 2)

            def body(i, carry, cols=cols):
                rows = pl.ds(pl.multiple_of(i * ROWS, ROWS), ROWS)
                dst[rows, cols] = (
                    f_own[rows, cols] + f32(f_recv[tick - 1, rows, cols])
                ).astype(jnp.bfloat16)
                return carry

            lax.fori_loop(0, tokens // ROWS, body, 0)

    def backward_product(load, dst):
        def body(n, carry):
            rows = pl.ds(pl.multiple_of(n * TILE, TILE), TILE)
            dst[:, rows] = lax.dot_general(
                load(), w[rows, :], CONTRACT_LAST, preferred_element_type=jnp.float32
            ).astype(jnp.bfloat16)
            return carry

        lax.fori_loop(0, w.shape[0] // TILE, body, 0)

    def add_halves(whole, received, store):
        def body(i, carry):
            rows = pl.ds(pl.multiple_of(i * ROWS, ROWS), ROWS)
            full = pl.ds(pl.multiple_of(t * half + i * ROWS, ROWS), ROWS)
            store(rows, (f32(whole[full, :]) + f32(received[rows, :])).astype(jnp.bfloat16))
            return carry

        lax.fori_loop(0, half // ROWS, body, 0)

    def backward_other(cotangent, tick):
        k = tick - 1
        backward_product(lambda: cotangent[...], pb.at[k])
        copy = remote("pb", pb.at[k, theirs], pbr.at[k], partner, tick)
        copy.start()
        return copy

    def backward_send(copy, tick):
        k = tick - 1
        copy.wait_recv()

        def store(rows, value):
            sb[k, rows, :] = value

        add_halves(pb.at[k], pbr.at[k], store)
        out = remote("dn", sb.at[k], dn.at[k, d], peer, tick)
        out.start()
        return out

    def backward_own(cotangent, tick):
        k = tick - 1
        backward_product(lambda: cotangent[t], po.at[k])
        copy = remote("po", po.at[k, theirs], por.at[k], partner, tick)
        copy.start()
        return copy

    def low_rank(cotangent, tick):
        gradient = (
            lax.dot_general(
                cotangent[0], upf[0], CONTRACT_LAST, preferred_element_type=jnp.float32
            )
            + lax.dot_general(
                cotangent[1], upf[1], CONTRACT_LAST, preferred_element_type=jnp.float32
            )
        ).astype(jnp.bfloat16)
        part = jnp.where(t == 0, gradient[:half], gradient[half:])
        for b in range(2):

            def body(n, carry, b=b):
                cols = pl.ds(pl.multiple_of(n * TILE, TILE), TILE)
                lora[b, :, cols] = ADAPTER_SCALE * lax.dot_general(
                    part, downf[b, cols, :], CONTRACT_LAST, preferred_element_type=jnp.float32
                )
                return carry

            lax.fori_loop(0, width // TILE, body, 0)
        return lax.dot_general(
            cotangent[0], projf[0], CONTRACT_LAST, preferred_element_type=jnp.float32
        ) + lax.dot_general(
            cotangent[1], projf[1], CONTRACT_LAST, preferred_element_type=jnp.float32
        )

    def backward_finish(copy_own, copy_dn, hidden, inv, cotangent, dst, tick):
        k = tick - 1
        copy_own.wait_recv()

        def store(rows, value):
            dn[k, d, rows, :] = value

        add_halves(po.at[k], por.at[k], store)
        copy_dn.wait_recv()

        def body(i, carry):
            rows = pl.ds(pl.multiple_of(i * ROWS, ROWS), ROWS)
            full = pl.ds(pl.multiple_of(t * half + i * ROWS, ROWS), ROWS)
            scale = inv[full, :][:, :1]
            total = jnp.zeros((ROWS, 1), jnp.float32)
            for b in range(2):
                scaled = f32(nwf[b]) * (f32(dn[k, b, rows, :]) + lora[b, rows, :])
                lora[b, rows, :] = scaled
                total = total + jnp.sum(f32(hidden[b, full, :]) * scaled, axis=1, keepdims=True)
            factor = scale * scale * (total / features)
            for b in range(2):
                dst[b, rows, :] = (
                    f32(cotangent[b, full, :])
                    + scale * (lora[b, rows, :] - f32(hidden[b, full, :]) * factor)
                ).astype(jnp.bfloat16)
            return carry

        lax.fori_loop(0, half // ROWS, body, 0)

    def sketch(adapter, cols, tick):
        ranks, width_k = adapter.shape[1], cols.shape[1]
        piece = sk.shape[2]
        row = lax.broadcasted_iota(jnp.int32, (8, tokens), 0)
        place = lax.broadcasted_iota(jnp.int32, (8, tokens), 1)
        member = jnp.zeros((8, tokens), jnp.float32)
        start = jnp.int32(0)
        for j in range(segs):
            stop = start + counts[0, j, s + tick - 1]
            inside = (row == (tick - 1) * segs + j) & (place >= start) & (place < stop)
            member = member + jnp.where(inside, ADAPTER_SCALE, 0.0)
            start = stop
        member = member.astype(jnp.bfloat16)
        col_k = lax.broadcasted_iota(jnp.int32, (width_k, piece), 1)
        row_k = lax.broadcasted_iota(jnp.int32, (width_k, piece), 0)
        spread = (lax.rem(col_k, width_k) == row_k).astype(jnp.float32).astype(jnp.bfloat16)
        wide_cols = jnp.dot(
            cols.astype(jnp.bfloat16), spread, preferred_element_type=jnp.float32
        )
        row_r = lax.broadcasted_iota(jnp.int32, (ranks, piece), 0)
        col_r = lax.broadcasted_iota(jnp.int32, (ranks, piece), 1)

        for o in range(sections):
            first = o * (piece // width_k)
            pick = (row_r == first + lax.div(col_r, width_k)).astype(jnp.float32)
            wide = jnp.dot(adapter, pick.astype(jnp.bfloat16), preferred_element_type=jnp.float32)
            value = jnp.dot(
                member, (wide * wide_cols).astype(jnp.bfloat16), preferred_element_type=jnp.float32
            )
            sk[o] = value if tick == 1 else sk[o] + value

    local[0].wait()
    local[1].wait()
    normc.wait_recv()
    h1c.wait_recv()
    nin1 = forward_send(h1f, inv_f, 1)
    local[2].wait()
    s1c.wait_recv()
    normalize_into(s1f, inv_1, scratch_n)
    local[4].wait()
    downc.wait_recv()
    adapter_f1 = both(normed, downf).astype(jnp.bfloat16)
    adapter_s1 = both(scratch_n, downf).astype(jnp.bfloat16)
    for i in (3, 5, 6):
        local[i].wait()
    g1c.wait_recv()
    upc.wait_recv()
    projc.wait_recv()
    cols1 = low_rank(g1f, 1)
    local[8].wait()
    g1y.wait_recv()
    pb1 = backward_other(g1o, 1)
    nfw1 = forward_relay(nin1, 1)
    dn1 = backward_send(pb1, 1)
    fout1 = forward_other(nfw1, 1)
    po1 = backward_own(g1f, 1)
    backward_finish(po1, dn1, s1f, inv_1, g1f, bk, 1)
    down_stream = {"section": lax.rem(s + final, sections)}
    shift_b = [
        remote("shift_b", bk.at[b], g2f.at[b, mine], down_stream, b) for b in range(2)
    ]

    @pl.when(s > 0)
    def _():
        for copy in shift_b:
            copy.start()

    forward_own(h1f, adapter_f1)
    sketch(adapter_s1, cols1, 1)
    forward_finish(fout1, o1, 1)
    shift_f = remote("shift_f", o1, h2f.at[t], {"section": lax.rem(s + 1, sections)})

    @pl.when(s < final)
    def _():
        shift_f.start()

    @pl.when(s == final)
    def _():
        last_copy.wait()
        lastc.wait_recv()

    g2c = [
        remote("g2", g2f.at[b, mine], g2f.at[b, mine], partner, b) for b in range(2)
    ]
    first_y = COPIES.index("g2y0")
    g2y = [
        pltpu.make_async_remote_copy(
            src_ref=g2f.at[b, mine],
            dst_ref=g2o.at[mine],
            send_sem=send_sem.at[first_y + b],
            recv_sem=recv_sem.at[first_y + t],
            device_id={"dp": other_d, "tensor": b},
            device_id_type=MESH,
        )
        for b in range(2)
    ]
    for b in range(2):

        @pl.when(s < final)
        def _(b=b):
            shift_b[b].wait_recv()

        g2y[b].start()

        @pl.when(s < final)
        def _(b=b):
            g2c[b].start()

    local[7].wait()
    s2c.wait_recv()
    normalize_into(s2f, inv_2, scratch_n)
    adapter_s2 = both(scratch_n, downf).astype(jnp.bfloat16)

    @pl.when(s < final)
    def _():
        for copy in g2c:
            copy.wait_recv()

    @pl.when(s > 0)
    def _():
        for copy in shift_b:
            copy.wait_send()

    cols2 = low_rank(g2f, 2)
    nin1.wait_send()

    @pl.when(s > 0)
    def _():
        shift_f.wait_recv()

    @pl.when(s == 0)
    def _():
        enter_copy.wait()

    h2c = remote("h2", h2f.at[t], h2f.at[t], partner)
    h2c.start()
    h2c.wait_recv()
    nin2 = forward_send(h2f, inv_f, 2)
    adapter_f2 = both(normed, downf).astype(jnp.bfloat16)
    for b in range(2):
        pltpu.make_async_remote_copy(
            src_ref=g2f.at[b, mine],
            dst_ref=g2o.at[pl.ds(b * half, half)],
            send_sem=send_sem.at[first_y + b],
            recv_sem=recv_sem.at[first_y + b],
            device_id=peer,
            device_id_type=MESH,
        ).wait_recv()
    pb2 = backward_other(g2o, 2)
    nfw2 = forward_relay(nin2, 2)
    dn2 = backward_send(pb2, 2)
    fout2 = forward_other(nfw2, 2)
    po2 = backward_own(g2f, 2)
    sketch(adapter_s2, cols2, 2)
    sk_copies = []
    for step in range(1, sections):
        owner = lax.rem(s + step, sections)
        copy = pltpu.make_async_remote_copy(
            src_ref=sk.at[owner],
            dst_ref=skr.at[s],
            send_sem=sk_send.at[step],
            recv_sem=sk_recv.at[step],
            device_id={"section": owner},
            device_id_type=MESH,
        )
        copy.start()
        sk_copies.append(copy)
    skr[s] = sk[s]

    backward_finish(po2, dn2, s2f, inv_2, g2f, bk, 2)
    back = remote("back", bk.at[other_t], bkr, partner)
    back.start()
    forward_own(h2f, adapter_f2)
    out_b[mine, :] = bk[t]

    for copy in sk_copies:
        copy.wait_recv()
    batches = owners.shape[1]
    own_row = lax.broadcasted_iota(jnp.int32, (batches, batches), 0)
    onehot = (own_row == owners[...]).astype(jnp.float32)
    from_row = lax.broadcasted_iota(jnp.int32, (batches, 8 * sections), 0)
    from_col = lax.broadcasted_iota(jnp.int32, (batches, 8 * sections), 1)
    entry = lax.rem(from_col, 8)
    source = (
        (from_row == segs * lax.div(from_col, 8) + entry) & (entry < 2 * segs)
    ).astype(jnp.float32)
    table = jnp.dot(onehot, source, preferred_element_type=jnp.float32)
    out_s[...] = jnp.dot(
        table,
        skr[...].reshape(8 * sections, -1),
        precision=lax.Precision.HIGHEST,
        preferred_element_type=jnp.float32,
    )
    back.wait_recv()
    out_b[theirs, :] = bkr[...]
    forward_finish(fout2, out_f, 2)

    for copy in early + sk_copies + [
        h2c, nfw1, nin2, nfw2, pb1, pb2, dn1, dn2, po1, po2, back
    ] + fout1 + fout2 + g2y:
        copy.wait_send()

    @pl.when(s < final)
    def _():
        shift_f.wait_send()
        for copy in g2c:
            copy.wait_send()

    @pl.when(s == final)
    def _():
        lastc.wait_send()


def stationary(
    forward_input,
    entering_input,
    stored_input,
    output_gradient,
    last_gradient,
    norm_weight,
    frozen_weight,
    adapter_down,
    adapter_up,
    project,
    example_token_counts,
    sketch_owner_rows,
):
    sections = lax.axis_size("section")
    _, tokens, width = forward_input.shape
    rows = frozen_weight.shape[1]
    ranks, sketch_k = adapter_down.shape[2], project.shape[2]
    piece = ranks * sketch_k // sections
    half = tokens // 2
    bf, f = jnp.bfloat16, jnp.float32
    anywhere = pl.BlockSpec(memory_space=pl.ANY)
    vmem = pl.BlockSpec(memory_space=pltpu.VMEM)
    smem = pl.BlockSpec(memory_space=pltpu.SMEM)
    full = pltpu.VMEM((2, tokens, width), bf)
    outs = pl.pallas_call(
        functools.partial(window_kernel, sections),
        out_shape=(
            jax.ShapeDtypeStruct((tokens, width), bf),
            jax.ShapeDtypeStruct((tokens, width), bf),
            jax.ShapeDtypeStruct((sketch_owner_rows.shape[1], piece), f),
        ),
        in_specs=[anywhere] * 10 + [smem, vmem],
        out_specs=(vmem, vmem, vmem),
        scratch_shapes=[
            pltpu.VMEM((rows, width), bf),
            pltpu.VMEM((2, 1, width), bf),
            pltpu.VMEM((2, width, ranks), bf),
            pltpu.VMEM((2, ranks, width), bf),
            pltpu.VMEM((2, sketch_k, width), bf),
            full,
            full,
            full,
            full,
            full,
            full,
            pltpu.VMEM((tokens, width), bf),
            pltpu.VMEM((tokens, width), bf),
            full,
            full,
            full,
            full,
            full,
            pltpu.VMEM((tokens, width), f),
            pltpu.VMEM((tokens, width), bf),
            full,
            pltpu.VMEM((2, half, width), bf),
            full,
            pltpu.VMEM((2, half, width), bf),
            pltpu.VMEM((2, half, width), bf),
            pltpu.VMEM((2, 2, half, width), bf),
            pltpu.VMEM((2, half, width), f),
            pltpu.VMEM((2, half, width), bf),
            pltpu.VMEM((half, width), bf),
            pltpu.VMEM((tokens, 128), f),
            pltpu.VMEM((tokens, 128), f),
            pltpu.VMEM((tokens, 128), f),
            pltpu.VMEM((sections, 8, piece), f),
            pltpu.VMEM((sections, 8, piece), f),
            pltpu.SemaphoreType.DMA((len(COPIES),)),
            pltpu.SemaphoreType.DMA((len(COPIES),)),
            pltpu.SemaphoreType.DMA((sections,)),
            pltpu.SemaphoreType.DMA((sections,)),
            pltpu.SemaphoreType.DMA((11,)),
        ],
        compiler_params=pltpu.CompilerParams(
            collective_id=0, has_side_effects=True, vmem_limit_bytes=60 * 1024 * 1024
        ),
        name="window",
    )(
        forward_input[0],
        entering_input,
        stored_input[:, 0],
        output_gradient[0],
        last_gradient,
        norm_weight,
        frozen_weight[0],
        adapter_down[0],
        adapter_up[0],
        project[0].T,
        jnp.swapaxes(example_token_counts, 1, 2),
        sketch_owner_rows,
    )
    return outs[0][None], outs[1][None], outs[2]


def solution(mesh):
    placed = (
        P("section", "dp", "tensor"),
        P("dp", "tensor"),
        P(None, "section", "dp", "tensor"),
        P("section", "dp", "tensor"),
        P("dp", "tensor"),
        P("section", "tensor"),
        P("section", "dp", "tensor"),
        P("section", "tensor", None),
        P("section", None, "tensor"),
        P("section", "tensor", None),
        P("dp", None, None),
        P("dp", None),
    )
    shape = mesh.shape
    fits = shape['tensor'] == 2 and shape['dp'] == 2 and shape['section'] > 1
    return jax.shard_map(
        stationary if fits else per_device,
        mesh=mesh,
        in_specs=placed,
        out_specs=(P("section", "dp", "tensor"), P("section", "dp", "tensor"), P("dp", "section")),
        check_vma=False,
    )
```
